16 devices in a mesh: dp: 2 (over z), tp: 8 (over y, x, core).
Axes of the slice: x: 2, y: 2, z: 2, core: 2. Of those that a mesh axis runs over, the one named last changes fastest.
Arguments:
- tokens: bfloat16 [2, 2048, 4096], P('dp', 'tp'), parts along dimension 0
- start_pos: int32 [2], P('dp'), parts along dimension 0
- cos_tab: float32 [2, 2048, 128], P('dp'), parts along dimension 0
- sin_tab: float32 [2, 2048, 128], P('dp'), parts along dimension 0
- key_cache: bfloat16 [2, 2, 4096, 8, 128], P(None, 'dp', None, 'tp'), parts along dimension 1
- value_cache: bfloat16 [2, 2, 4096, 8, 128], P(None, 'dp', None, 'tp'), parts along dimension 1
- slot_pos: int32 [2, 4096], P('dp'), parts along dimension 0
- norm_params: bfloat16 [2, 4, 4096], replicated
- w_q: bfloat16 [2, 4096, 4096], P(None, None, 'tp')
- b_q: bfloat16 [2, 4096], P(None, 'tp')
- w_k: bfloat16 [2, 4096, 1024], P(None, None, 'tp')
- b_k: bfloat16 [2, 1024], P(None, 'tp')
- w_v: bfloat16 [2, 4096, 1024], P(None, None, 'tp')
- b_v: bfloat16 [2, 1024], P(None, 'tp')
- w_o: bfloat16 [2, 4096, 4096], P(None, 'tp')
- b_o: bfloat16 [2, 4096], replicated
- w_up: bfloat16 [2, 4096, 14336], P(None, None, 'tp')
- b_up: bfloat16 [2, 14336], P(None, 'tp')
- w_down: bfloat16 [2, 14336, 4096], P(None, 'tp')
- b_down: bfloat16 [2, 4096], replicated
Outputs:
- output 1: bfloat16 [2, 2048, 4096], P('dp', 'tp'), parts along dimension 0
- output 2: bfloat16 [2, 2, 4096, 8, 128], P(None, 'dp', None, 'tp'), parts along dimension 1
- output 3: bfloat16 [2, 2, 4096, 8, 128], P(None, 'dp', None, 'tp'), parts along dimension 1
- output 4: int32 [2, 4096], P('dp'), parts along dimension 0
There are 2 independent parts. The reference program is written for one: setup_inputs(seed, part) draws one part's arguments, and reference() takes and returns one part's arrays. A program takes and returns all parts, laid end to end along the dimension named above; an argument that names none is the same for every part.
All inputs are finite; a program needn't handle non-finite values.
Results may differ from the reference program's by a relative error of at most 0.02.
Values are sent between devices in bfloat16 or wider.
A program may use at most 1 GiB of HBM per device.

```python
import jax
import jax.numpy as jnp
from jax import lax

NUM_SEQS = 1
CHUNK_LEN = 2048
MODEL_DIM = 4096
NUM_HEADS = 32
KV_HEADS = 8
HEAD_DIM = 128
FFN_DIM = 14336
WINDOW = 4096
NUM_LAYERS = 2
NORM_EPS = 1e-5
ROPE_BASE = 1000000.0


def draw_positions(start_key):
    drawn = jax.random.randint(start_key, (NUM_SEQS,), 0, 3 * WINDOW)
    start_pos = jnp.where(jnp.arange(NUM_SEQS) == 0, drawn % WINDOW, drawn).astype(jnp.int32)
    slots = jnp.arange(WINDOW)
    latest = start_pos[:, None] - 1 - (start_pos[:, None] - 1 - slots[None, :]) % WINDOW
    slot_pos = jnp.where(latest >= 0, latest, -1).astype(jnp.int32)
    return start_pos, slot_pos


def rotary_tables(start_pos):
    positions = (start_pos[:, None] + jnp.arange(CHUNK_LEN)[None, :]).astype(jnp.float32)
    inv_freq = ROPE_BASE ** (-jnp.arange(0, HEAD_DIM, 2).astype(jnp.float32) / HEAD_DIM)
    angles = positions[:, :, None] * inv_freq[None, None, :]
    angles = jnp.concatenate([angles, angles], axis=-1)
    return jnp.cos(angles), jnp.sin(angles)


def normal_draw(key, shape, scale):
    return (jax.random.normal(key, shape, jnp.float32) * scale).astype(jnp.bfloat16)


def setup_inputs(seed: int = 0, part: int = 0) -> dict:
    part_keys = jax.random.split(jax.random.fold_in(jax.random.key(seed), part), 4)
    weight_keys = jax.random.split(jax.random.key(seed + 1), 13)
    start_pos, slot_pos = draw_positions(part_keys[1])
    cos_tab, sin_tab = rotary_tables(start_pos)
    cache_shape = (NUM_LAYERS, NUM_SEQS, WINDOW, KV_HEADS, HEAD_DIM)
    q_width = NUM_HEADS * HEAD_DIM
    kv_width = KV_HEADS * HEAD_DIM
    norm_base = jnp.array([1.0, 0.0, 1.0, 0.0], jnp.float32)[None, :, None]
    norm_spread = jnp.array([0.25, 0.2, 0.25, 0.2], jnp.float32)[None, :, None]
    norm_noise = jax.random.normal(weight_keys[0], (NUM_LAYERS, 4, MODEL_DIM), jnp.float32)
    return {
        'tokens': normal_draw(part_keys[0], (NUM_SEQS, CHUNK_LEN, MODEL_DIM), 1.0),
        'start_pos': start_pos,
        'cos_tab': cos_tab,
        'sin_tab': sin_tab,
        'key_cache': normal_draw(part_keys[2], cache_shape, 1.0),
        'value_cache': normal_draw(part_keys[3], cache_shape, 1.0),
        'slot_pos': slot_pos,
        'norm_params': (norm_base + norm_spread * norm_noise).astype(jnp.bfloat16),
        'w_q': normal_draw(weight_keys[1], (NUM_LAYERS, MODEL_DIM, q_width), 2.5 * MODEL_DIM ** -0.5),
        'b_q': normal_draw(weight_keys[2], (NUM_LAYERS, q_width), 0.5),
        'w_k': normal_draw(weight_keys[3], (NUM_LAYERS, MODEL_DIM, kv_width), MODEL_DIM ** -0.5),
        'b_k': normal_draw(weight_keys[4], (NUM_LAYERS, kv_width), 0.5),
        'w_v': normal_draw(weight_keys[5], (NUM_LAYERS, MODEL_DIM, kv_width), MODEL_DIM ** -0.5),
        'b_v': normal_draw(weight_keys[6], (NUM_LAYERS, kv_width), 0.5),
        'w_o': normal_draw(weight_keys[7], (NUM_LAYERS, q_width, MODEL_DIM), 2.0 * q_width ** -0.5),
        'b_o': normal_draw(weight_keys[8], (NUM_LAYERS, MODEL_DIM), 0.3),
        'w_up': normal_draw(weight_keys[9], (NUM_LAYERS, MODEL_DIM, FFN_DIM), MODEL_DIM ** -0.5),
        'b_up': normal_draw(weight_keys[10], (NUM_LAYERS, FFN_DIM), 0.5),
        'w_down': normal_draw(weight_keys[11], (NUM_LAYERS, FFN_DIM, MODEL_DIM), FFN_DIM ** -0.5),
        'b_down': normal_draw(weight_keys[12], (NUM_LAYERS, MODEL_DIM), 0.3),
    }


def layer_norm(hidden, gain, shift):
    values = hidden.astype(jnp.float32)
    centered = values - jnp.mean(values, axis=-1, keepdims=True)
    variance = jnp.mean(centered * centered, axis=-1, keepdims=True)
    scaled = centered * lax.rsqrt(variance + NORM_EPS)
    return (scaled * gain.astype(jnp.float32) + shift.astype(jnp.float32)).astype(jnp.bfloat16)


def apply_rotary(values, cos_b, sin_b):
    half = values.shape[-1] // 2
    turned = jnp.concatenate([-values[..., half:], values[..., :half]], axis=-1)
    return (values * cos_b + turned * sin_b).astype(jnp.bfloat16)


def attend_group(group_in, old_ok, new_ok):
    query, key_new, value_new, cache_k, cache_v = group_in
    scale = HEAD_DIM ** -0.5
    score_old = jnp.einsum('gcd,wd->gcw', query.astype(jnp.float32), cache_k.astype(jnp.float32)) * scale
    score_new = jnp.einsum('gcd,jd->gcj', query.astype(jnp.float32), key_new.astype(jnp.float32)) * scale
    score_old = jnp.where(old_ok[None], score_old, -jnp.inf)
    score_new = jnp.where(new_ok[None], score_new, -jnp.inf)
    top = jnp.maximum(jnp.max(score_old, axis=-1, keepdims=True), jnp.max(score_new, axis=-1, keepdims=True))
    exp_old = jnp.exp(score_old - top)
    exp_new = jnp.exp(score_new - top)
    total = jnp.sum(exp_old, axis=-1, keepdims=True) + jnp.sum(exp_new, axis=-1, keepdims=True)
    mixed = jnp.einsum('gcw,wd->gcd', exp_old.astype(jnp.bfloat16).astype(jnp.float32), cache_v.astype(jnp.float32))
    mixed = mixed + jnp.einsum('gcj,jd->gcd', exp_new.astype(jnp.bfloat16).astype(jnp.float32), value_new.astype(jnp.float32))
    return (mixed / total).astype(jnp.bfloat16)


def attend_sequence(seq_inputs):
    query, key_new, value_new, cache_k, cache_v, held_pos, first_pos = seq_inputs
    positions = first_pos + jnp.arange(CHUNK_LEN)
    old_ok = (held_pos[None, :] >= 0) & (held_pos[None, :] > positions[:, None] - WINDOW) & (held_pos[None, :] <= positions[:, None])
    new_ok = jnp.arange(CHUNK_LEN)[None, :] <= jnp.arange(CHUNK_LEN)[:, None]
    grouped = query.reshape(CHUNK_LEN, KV_HEADS, NUM_HEADS // KV_HEADS, HEAD_DIM).transpose(1, 2, 0, 3)
    per_group = lax.map(lambda group_in: attend_group(group_in, old_ok, new_ok), (grouped, key_new.transpose(1, 0, 2), value_new.transpose(1, 0, 2), cache_k.transpose(1, 0, 2), cache_v.transpose(1, 0, 2)))
    return per_group.transpose(2, 0, 1, 3).reshape(CHUNK_LEN, NUM_HEADS * HEAD_DIM)


def reference(tokens, start_pos, cos_tab, sin_tab, key_cache, value_cache, slot_pos, norm_params, w_q, b_q, w_k, b_k, w_v, b_v, w_o, b_o, w_up, b_up, w_down, b_down):
    positions = start_pos[:, None] + jnp.arange(CHUNK_LEN)[None, :]
    slots = positions % WINDOW
    rows = jnp.arange(NUM_SEQS)[:, None]
    cos_b = cos_tab[:, :, None, :]
    sin_b = sin_tab[:, :, None, :]
    tok_count = NUM_SEQS * CHUNK_LEN

    def layer_step(hidden, layer_in):
        cache_k, cache_v, norms, proj_q, bias_q, proj_k, bias_k, proj_v, bias_v, proj_o, bias_o, proj_up, bias_up, proj_down, bias_down = layer_in
        normed = layer_norm(hidden, norms[0], norms[1]).reshape(tok_count, MODEL_DIM)
        query = jnp.dot(normed, proj_q, preferred_element_type=jnp.float32) + bias_q.astype(jnp.float32)
        query = apply_rotary(query.reshape(NUM_SEQS, CHUNK_LEN, NUM_HEADS, HEAD_DIM), cos_b, sin_b)
        key_new = jnp.dot(normed, proj_k, preferred_element_type=jnp.float32) + bias_k.astype(jnp.float32)
        key_new = apply_rotary(key_new.reshape(NUM_SEQS, CHUNK_LEN, KV_HEADS, HEAD_DIM), cos_b, sin_b)
        value_new = (jnp.dot(normed, proj_v, preferred_element_type=jnp.float32) + bias_v.astype(jnp.float32)).astype(jnp.bfloat16)
        value_new = value_new.reshape(NUM_SEQS, CHUNK_LEN, KV_HEADS, HEAD_DIM)
        mixed = lax.map(attend_sequence, (query, key_new, value_new, cache_k, cache_v, slot_pos, start_pos))
        attended = jnp.dot(mixed.reshape(tok_count, NUM_HEADS * HEAD_DIM), proj_o, preferred_element_type=jnp.float32)
        middle = (hidden.astype(jnp.float32) + attended.reshape(NUM_SEQS, CHUNK_LEN, MODEL_DIM) + bias_o.astype(jnp.float32)).astype(jnp.bfloat16)
        normed = layer_norm(middle, norms[2], norms[3]).reshape(tok_count, MODEL_DIM)
        lifted = jnp.dot(normed, proj_up, preferred_element_type=jnp.float32) + bias_up.astype(jnp.float32)
        active = jax.nn.gelu(lifted, approximate=True).astype(jnp.bfloat16)
        lowered = jnp.dot(active, proj_down, preferred_element_type=jnp.float32).reshape(NUM_SEQS, CHUNK_LEN, MODEL_DIM)
        layer_out = (middle.astype(jnp.float32) + lowered + bias_down.astype(jnp.float32)).astype(jnp.bfloat16)
        new_k = cache_k.at[rows, slots].set(key_new)
        new_v = cache_v.at[rows, slots].set(value_new)
        return layer_out, (new_k, new_v)

    final, (key_out, value_out) = lax.scan(layer_step, tokens, (key_cache, value_cache, norm_params, w_q, b_q, w_k, b_k, w_v, b_v, w_o, b_o, w_up, b_up, w_down, b_down))
    pos_out = slot_pos.at[rows, slots].set(positions.astype(jnp.int32))
    return final, key_out, value_out, pos_out
```

```python
import functools

import jax
import jax.numpy as jnp
from jax import lax
from jax.experimental import pallas as pl
from jax.experimental.pallas import tpu as pltpu
from jax.sharding import PartitionSpec as P

NORM_EPS = 1e-5
CHUNKS = 2
MASKED = -1e30
LOG2_E = 1.4426950408889634
VMEM_LIMIT = 56 * 2**20
ANY = pl.BlockSpec(memory_space=pl.ANY)
SMEM = pl.BlockSpec(memory_space=pltpu.SMEM)
VMEM = pl.BlockSpec(memory_space=pltpu.VMEM)
ORDER = ((0, 2, 4, 6, 1, 5, 3, 7), (0, 4, 2, 6, 1, 3, 5, 7))
FIRST = [(i, i ^ (4 if i % 2 else 2)) for i in range(8)]
SECOND = [(i, i ^ (2 if i % 2 else 4)) for i in range(8)]
PARTNER = [(i, i ^ 1) for i in range(8)]


def params():
    return pltpu.CompilerParams(vmem_limit_bytes=VMEM_LIMIT)


def cost(flops, nbytes, trans=0):
    return pl.CostEstimate(flops=int(flops), bytes_accessed=int(nbytes), transcendentals=int(trans))


def layer_norm(hidden, gain, shift):
    values = hidden.astype(jnp.float32)
    centered = values - jnp.mean(values, axis=-1, keepdims=True)
    variance = jnp.mean(centered * centered, axis=-1, keepdims=True)
    scaled = centered * lax.rsqrt(variance + NORM_EPS)
    return (scaled * gain.astype(jnp.float32) + shift.astype(jnp.float32)).astype(jnp.bfloat16)


def send(block, pairs):
    return lax.ppermute(block, 'tp', pairs)


def gather(block):
    near = send(block, FIRST)
    side = send(block, SECOND)
    far = send(near, SECOND)
    mine = [block, near, side, far]
    return mine + [send(each, PARTNER) for each in mine]


def start_copies(blocks, acts, sems):
    rows = blocks[0].shape[0]
    return [pltpu.make_async_copy(ref, acts.at[pl.ds(s * rows, rows)], sems.at[s]) for s, ref in enumerate(blocks)]


def qkv_kernel(pos_ref, *refs, heads, dim):
    blocks, rest = refs[:8], refs[8:]
    wq_ref, bq_ref, wk_ref, bk_ref, wv_ref, bv_ref, cos_ref, sin_ref, q_ref, k_ref, v_ref, acts, sems = rest
    rows = blocks[0].shape[0]
    step = pl.program_id(0)
    per = q_ref.shape[0]
    copies = start_copies(blocks, acts, sems)

    @pl.when(step == 0)
    def _():
        for copy in copies:
            copy.start()

    for t in range(8 // per):
        @pl.when(step == t)
        def _():
            for copy in copies[t * per:(t + 1) * per]:
                copy.wait()

    a = acts[pl.ds(pl.multiple_of(step * (per * rows), per * rows), per * rows), :]
    q = jnp.dot(a, wq_ref[0], preferred_element_type=jnp.float32) + bq_ref[0].astype(jnp.float32)
    k = jnp.dot(a, wk_ref[0], preferred_element_type=jnp.float32) + bk_ref[0].astype(jnp.float32)
    v = jnp.dot(a, wv_ref[0], preferred_element_type=jnp.float32) + bv_ref[0].astype(jnp.float32)
    sign = jnp.where(lax.broadcasted_iota(jnp.int32, (rows, dim), 1) < dim // 2, -1.0, 1.0)
    for s in range(per):
        part = slice(s * rows, (s + 1) * rows)
        first = pl.multiple_of(pos_ref[step * per + s], rows)
        cos = cos_ref[pl.ds(first, rows), :]
        sin = sin_ref[pl.ds(first, rows), :] * sign
        dest = pl.ds(pl.multiple_of(pos_ref[8 + step * per + s], rows), rows)

        def rotary(u):
            return (u * cos + pltpu.roll(u, dim // 2, 1) * sin).astype(jnp.bfloat16)

        for h in range(heads):
            q_ref[s, h * rows:(h + 1) * rows, :] = rotary(q[part, h * dim:(h + 1) * dim])
        k_ref[dest, :] = rotary(k[part])
        v_ref[dest, :] = v[part].astype(jnp.bfloat16)


def qkv(blocks, pos, layer, w_q, b_q, w_k, b_k, w_v, b_v, cos_tab, sin_tab):
    rows, width = blocks[0].shape
    dim = cos_tab.shape[1]
    heads = w_q.shape[2] // dim
    per = 2
    full = lambda arr: pl.BlockSpec((1,) + arr.shape[1:], lambda s: (layer,) + (0,) * (arr.ndim - 1))
    whole = lambda shape: pl.BlockSpec(shape, lambda s: (0,) * len(shape))
    return pl.pallas_call(
        functools.partial(qkv_kernel, heads=heads, dim=dim),
        grid=(8 // per,),
        in_specs=[SMEM] + [ANY] * 8 + [full(x) for x in (w_q, b_q, w_k, b_k, w_v, b_v)] + [whole(cos_tab.shape)] * 2,
        out_specs=[pl.BlockSpec((per, heads * rows, dim), lambda s: (s, 0, 0)), whole((8 * rows, dim)), whole((8 * rows, dim))],
        out_shape=[jax.ShapeDtypeStruct((8, heads * rows, dim), jnp.bfloat16)] + [jax.ShapeDtypeStruct((8 * rows, dim), jnp.bfloat16)] * 2,
        scratch_shapes=[pltpu.VMEM((8 * rows, width), jnp.bfloat16), pltpu.SemaphoreType.DMA((8,))],
        compiler_params=params(),
        cost_estimate=cost(2 * 8 * rows * width * (heads + 2) * dim, 2 * width * (8 * rows + (heads + 2) * dim)),
        name='qkv',
    )(pos, *blocks, w_q, b_q, w_k, b_k, w_v, b_v, cos_tab, sin_tab)


def attend_kernel(pos_ref, q_ref, k_ref, v_ref, o_ref, acc_ref, m_ref, l_ref, sa_ref, sb_ref, *, window, bk, group, rows):
    j0 = pos_ref[pl.program_id(0)]
    first = pos_ref[16]
    dim = q_ref.shape[2]
    scale = (dim ** -0.5) * LOG2_E
    m_ref[...] = jnp.full(m_ref.shape, MASKED, jnp.float32)
    l_ref[...] = jnp.zeros(l_ref.shape, jnp.float32)
    acc_ref[...] = jnp.zeros(acc_ref.shape, jnp.float32)
    low = jnp.maximum(j0, first) // bk
    high = (window + j0) // bk

    def scores(b):
        keys = k_ref[pl.ds(pl.multiple_of(b * bk, bk), bk), :]
        return lax.dot_general(q_ref[0], keys, (((1,), (1,)), ((), ())), preferred_element_type=jnp.float32)

    def mask(s, b):
        t = b * bk + lax.broadcasted_iota(jnp.int32, s.shape, 1)
        j = j0 + lax.broadcasted_iota(jnp.int32, s.shape, 0) % rows
        return jnp.where((t > j) & (t >= first) & (t <= j + window), s, MASKED)

    def update(s, b):
        m_old = m_ref[...]
        m_new = jnp.maximum(m_old, jnp.max(s, axis=1, keepdims=True) * scale)
        alpha = jnp.exp2(m_old - m_new)
        parts = [jnp.exp2(s[:, i * dim:(i + 1) * dim] * scale - m_new) for i in range(bk // dim)]
        total = l_ref[...] * alpha + functools.reduce(jnp.add, parts)
        p = jnp.concatenate([x.astype(jnp.bfloat16) for x in parts], axis=1)
        values = v_ref[pl.ds(pl.multiple_of(b * bk, bk), bk), :]
        return m_new, total, acc_ref[...] * alpha + jnp.dot(p, values, preferred_element_type=jnp.float32)

    def put(state):
        m_ref[...], l_ref[...], acc_ref[...] = state

    put(update(mask(scores(low), low), low))
    count = high - low - 1

    @pl.when(count > 0)
    def _():
        sa_ref[...] = scores(low + 1)

        def pair(i, carry):
            b = low + 1 + 2 * i
            s = sa_ref[...]
            later = scores(b + 1)
            state = update(s, b)
            sb_ref[...] = later
            put(state)
            s = sb_ref[...]
            later = scores(b + 2)
            state = update(s, b + 1)
            sa_ref[...] = later
            put(state)
            return carry

        lax.fori_loop(0, count // 2, pair, 0)

        @pl.when(count % 2 == 1)
        def _():
            put(update(sa_ref[...], high - 1))

    @pl.when(high > low)
    def _():
        put(update(mask(scores(high), high), high))

    out = (acc_ref[...] / jnp.sum(l_ref[...], axis=1, keepdims=True)).astype(jnp.bfloat16)
    for h in range(group):
        o_ref[:, h * dim:(h + 1) * dim] = out[h * rows:(h + 1) * rows]


def attend(pos, q, keys, values, window):
    slots, stacked, dim = q.shape
    group = 4
    rows = stacked // group
    bk = 512
    whole = pl.BlockSpec(keys.shape, lambda s: (0, 0))
    return pl.pallas_call(
        functools.partial(attend_kernel, window=window, bk=bk, group=group, rows=rows),
        grid=(slots,),
        in_specs=[SMEM, pl.BlockSpec((1, stacked, dim), lambda s: (s, 0, 0)), whole, whole],
        out_specs=pl.BlockSpec((rows, group * dim), lambda s: (s, 0)),
        out_shape=jax.ShapeDtypeStruct((slots * rows, group * dim), jnp.bfloat16),
        scratch_shapes=[pltpu.VMEM((stacked, dim), jnp.float32)] * 3 + [pltpu.VMEM((stacked, bk), jnp.float32)] * 2,
        compiler_params=params(),
        cost_estimate=cost(8 * slots * stacked * (window + bk) * dim, 2**22, slots * stacked * (window + bk)),
        name='attend',
    )(pos, q, keys, values)


def up_kernel(*refs):
    blocks, (w_ref, b_ref, o_ref, acts, sems) = refs[:8], refs[8:]
    copies = start_copies(blocks, acts, sems)

    @pl.when(pl.program_id(0) == 0)
    def _():
        for copy in copies:
            copy.start()
        for copy in copies:
            copy.wait()

    x = jnp.dot(acts[...], w_ref[0], preferred_element_type=jnp.float32) + b_ref[0].astype(jnp.float32)
    o_ref[...] = jax.nn.gelu(x, approximate=True).astype(jnp.bfloat16)


def up(blocks, layer, w_up, b_up):
    rows, width = blocks[0].shape
    cols = w_up.shape[2]
    bn = 256
    return pl.pallas_call(
        up_kernel,
        grid=(cols // bn,),
        in_specs=[ANY] * 8 + [pl.BlockSpec((1, width, bn), lambda n: (layer, 0, n)), pl.BlockSpec((1, 1, bn), lambda n: (layer, 0, n))],
        out_specs=pl.BlockSpec((8 * rows, bn), lambda n: (0, n)),
        out_shape=jax.ShapeDtypeStruct((8 * rows, cols), jnp.bfloat16),
        scratch_shapes=[pltpu.VMEM((8 * rows, width), jnp.bfloat16), pltpu.SemaphoreType.DMA((8,))],
        compiler_params=params(),
        cost_estimate=cost(2 * 8 * rows * width * cols, 2 * (width * (8 * rows + cols) + 8 * rows * cols), 8 * rows * cols),
        name='up',
    )(*blocks, w_up, b_up)


def lower_kernel(a_ref, w_ref, o_ref):
    o_ref[...] = jnp.dot(a_ref[...], w_ref[0], preferred_element_type=jnp.float32).astype(jnp.bfloat16)


def lower_add_kernel(a_ref, w_ref, r_ref, *o_refs):
    x = jnp.dot(a_ref[...], w_ref[0], preferred_element_type=jnp.float32) + r_ref[...].astype(jnp.float32)
    x = x.astype(jnp.bfloat16)
    rows = o_refs[0].shape[0]
    for s, o_ref in enumerate(o_refs):
        o_ref[...] = x[s * rows:(s + 1) * rows]


def lower(acts, layer, weight, received=None):
    half, depth = acts.shape[0] // 2, acts.shape[1]
    width = weight.shape[2]
    bn = 512
    rows = half // 4
    mine = received is not None
    specs = [pl.BlockSpec((half, depth), lambda n: (0 if mine else 1, 0)), pl.BlockSpec((1, depth, bn), lambda n: (layer, 0, n))]
    block = pl.BlockSpec((half, bn), lambda n: (0, n))
    price = cost(2 * half * depth * width, 2 * (depth * (half + width) + half * width * (2 if mine else 1)))
    if not mine:
        return pl.pallas_call(lower_kernel, grid=(width // bn,), in_specs=specs, out_specs=block,
                              out_shape=jax.ShapeDtypeStruct((half, width), jnp.bfloat16),
                              compiler_params=params(), cost_estimate=price, name='lower')(acts, weight)
    return pl.pallas_call(lower_add_kernel, grid=(width // bn,), in_specs=specs + [block],
                          out_specs=[pl.BlockSpec((rows, bn), lambda n: (0, n))] * 4,
                          out_shape=[jax.ShapeDtypeStruct((rows, width), jnp.bfloat16)] * 4,
                          compiler_params=params(), cost_estimate=price, name='lower_add')(acts, weight, received)


def add_pair(left, right):
    return (left.astype(jnp.float32) + right.astype(jnp.float32)).astype(jnp.bfloat16)


def scatter(acts, layer, weight):
    away = lower(acts, layer, weight)
    s0, s1, s2, s3 = lower(acts, layer, weight, send(away, PARTNER))
    t3 = send(s3, SECOND)
    t2 = send(s2, SECOND)
    t1 = send(add_pair(s1, t3), FIRST)
    return s0.astype(jnp.float32) + t2.astype(jnp.float32) + t1.astype(jnp.float32)


def turn(array, shift):
    size = array.shape[0]
    return lax.dynamic_slice_in_dim(jnp.concatenate([array, array], axis=0), (-shift) % size, size, axis=0)


def solution(mesh):
    assert mesh.shape['tp'] == 8
    row_spec = P('dp', 'tp', None)
    cache_spec = P(None, 'dp', None, 'tp', None)
    col_spec = P(None, None, 'tp')
    bias_spec = P(None, 'tp')
    in_specs = (row_spec, P('dp'), P('dp', None, None), P('dp', None, None), cache_spec, cache_spec, P('dp', None), P(), col_spec, bias_spec, col_spec, bias_spec, col_spec, bias_spec, P(None, 'tp', None), P(), col_spec, bias_spec, P(None, 'tp', None), P())
    out_specs = (row_spec, cache_spec, cache_spec, P('dp', None))

    def device_step(tokens, start_pos, cos_tab, sin_tab, key_cache, value_cache, slot_pos, norm_params, w_q, b_q, w_k, b_k, w_v, b_v, w_o, b_o, w_up, b_up, w_down, b_down):
        layers, _, window, _, dim = key_cache.shape
        chunk = cos_tab.shape[1]
        own = tokens.shape[1]
        rows = own // CHUNKS
        start = start_pos[0]
        me = lax.axis_index('tp')
        order = jnp.where(me % 2 == 0, jnp.array(ORDER[0], jnp.int32), jnp.array(ORDER[1], jnp.int32))
        source = me ^ order
        oldest = jnp.maximum(window - start, 0)[None]
        pos = [jnp.concatenate([source * own + c * rows, source * rows, oldest]).astype(jnp.int32) for c in range(CHUNKS)]
        cos, sin = cos_tab[0], sin_tab[0]
        lift = lambda bias: bias[:, None, :]
        hidden = [tokens[0, c * rows:(c + 1) * rows] for c in range(CHUNKS)]
        old = [[turn(cache[l, 0, :, 0, :], -start) for cache in (key_cache, value_cache)] for l in range(layers)]
        key_out, value_out = [], []

        def natural(parts):
            return jnp.stack([x.reshape(8, rows, dim) for x in parts], axis=1).reshape(chunk, dim)

        for l in range(layers):
            blocks = [gather(layer_norm(hidden[c], norm_params[l, 0], norm_params[l, 1])) for c in range(CHUNKS)]
            made = [qkv(blocks[c], pos[c], l, w_q, lift(b_q), w_k, lift(b_k), w_v, lift(b_v), cos, sin) for c in range(CHUNKS)]
            keys = jnp.concatenate([old[l][0], natural([x[1] for x in made])], axis=0)
            values = jnp.concatenate([old[l][1], natural([x[2] for x in made])], axis=0)
            middle = []
            for c in range(CHUNKS):
                mixed = attend(pos[c], made[c][0], keys, values, window)
                summed = scatter(mixed, l, w_o)
                middle.append((hidden[c].astype(jnp.float32) + summed + b_o[l].astype(jnp.float32)).astype(jnp.bfloat16))
            for c in range(CHUNKS):
                active = up(gather(layer_norm(middle[c], norm_params[l, 2], norm_params[l, 3])), l, w_up, lift(b_up))
                summed = scatter(active, l, w_down)
                hidden[c] = (middle[c].astype(jnp.float32) + summed + b_down[l].astype(jnp.float32)).astype(jnp.bfloat16)
            for out, both in ((key_out, keys), (value_out, values)):
                out.append(turn(both[chunk:], start + chunk)[None, :, None, :])
        offset = (jnp.arange(window) - start) % window
        pos_out = jnp.where(offset < chunk, start + offset, slot_pos[0])[None]
        return jnp.concatenate(hidden, axis=0)[None], jnp.stack(key_out), jnp.stack(value_out), pos_out.astype(jnp.int32)

    return jax.shard_map(device_step, mesh=mesh, in_specs=in_specs, out_specs=out_specs, check_vma=False)
```
